32 devices in a mesh: mc: 8 (over z, x), mr: 4 (over y, core).
Axes of the slice: x: 2, y: 2, z: 4, core: 2. Of those that a mesh axis runs over, the one named last changes fastest.
Arguments:
- column_panel: float32 [4096, 256], P('mc', 'mr'), may hold values from -0.375 to 0.375
- diag_block: float32 [256, 256], P('mc', 'mr'), may hold values from -4.3 to 4.3, as said below
- row_panel: float32 [256, 32768], P('mc', 'mr'), may hold values from -6 to 6
- trailing: float32 [4096, 32768], P('mc', 'mr'), may hold values from -6 to 6
Outputs:
- solved_panel: float32 [4096, 256], P('mc', 'mr')
- inverse_block: float32 [256, 256], P('mc', 'mr')
- scaled_panel: float32 [256, 32768], P('mc', 'mr')
- updated: float32 [4096, 32768], P('mc', 'mr')
The draws below stay inside these ranges and needn't reach their ends.
Inputs may be any that keep to these rules, and one draw needn't show every extreme that they name: `diag_block`: upper triangle with a diagonal of magnitude 2 to 4 and small off-diagonal entries.
All inputs are finite; a program needn't handle non-finite values.
Results may differ from the reference program's by a relative error of at most 0.00011.
Values sent between devices are 32-bit elements; how exact they have to be, the bound alone decides.
A program may use at most 128 MiB of HBM per device.

```python
import jax
import jax.numpy as jnp
from jax import lax

B = 256
COLS = 32768
ROWS = 4096


def draw_diag_block(key, part):
    first, second, third = jax.random.split(key, 3)
    offdiag = 0.06 * jnp.clip(jax.random.normal(first, (B, B), jnp.float32), -5.0, 5.0)
    signs = jnp.where(jax.random.bernoulli(second, 0.5, (B,)), 1.0, -1.0).astype(jnp.float32)
    magnitude = jax.random.uniform(third, (B,), jnp.float32, 2.0, 4.0)
    keep = 1.0 - jnp.eye(B, dtype=jnp.float32)
    return offdiag * keep + jnp.diag(signs * magnitude)


def shard_levels(rng, extent, cuts, smallest, largest):
    loudness = 1.0
    for position, parts in cuts:
        steps = jax.random.uniform(jax.random.fold_in(jax.random.fold_in(rng, 6), position), (parts,), jnp.float32, smallest / len(cuts), largest / len(cuts))
        loudness = loudness * jnp.repeat(jnp.exp(steps), extent[position] // parts).reshape((-1,) + (1,) * (len(extent) - 1 - position))
    return loudness


def centred(rng, shape, deviation, reach, pieces=(), kind=jnp.bfloat16):
    array = deviation * jax.random.normal(rng, shape, jnp.float32)
    if pieces:
        array = array * shard_levels(rng, shape, pieces, -0.22, 0.18)
    return jnp.clip(array, -reach, reach).astype(kind)


def setup_inputs(seed: int = 0) -> dict:
    key_of = jax.random.split(jax.random.key(seed), 5)
    column_panel = centred(key_of[0], (ROWS, B), B ** -0.5, 0.375, ((0, 8), (1, 4)), jnp.float32)
    diag_block = draw_diag_block(jax.random.fold_in(key_of[4], 71), 0)
    row_panel = centred(key_of[2], (B, COLS), 1.0, 6.0, ((0, 8), (1, 4)), jnp.float32)
    trailing = centred(key_of[3], (ROWS, COLS), 1.0, 6.0, ((0, 8), (1, 4)), jnp.float32)
    return {"column_panel": column_panel, "diag_block": diag_block, "row_panel": row_panel, "trailing": trailing}


def reference(column_panel, diag_block, row_panel, trailing):
    upper = jnp.triu(diag_block)
    identity = jnp.eye(B, dtype=diag_block.dtype)
    inverse_block = jax.scipy.linalg.solve_triangular(upper, identity, lower=False)
    solved_panel = -jnp.dot(column_panel, inverse_block, precision=lax.Precision.HIGHEST)
    updated = trailing + jnp.dot(solved_panel, row_panel, precision=lax.Precision.HIGHEST)
    scaled_panel = jnp.dot(inverse_block, row_panel, precision=lax.Precision.HIGHEST)
    return (solved_panel, inverse_block, scaled_panel, updated)
```

```python
import functools

import jax
import jax.numpy as jnp
from jax import lax
from jax.experimental import pallas as pl
from jax.experimental.pallas import tpu as pltpu
from jax.sharding import PartitionSpec as P

HIGHEST = lax.Precision.HIGHEST


def dot(a, b):
    return jnp.dot(a, b, precision=HIGHEST, preferred_element_type=jnp.float32)


def upper_inverse(matrix):
    order = matrix.shape[0]
    row = lax.broadcasted_iota(jnp.int32, (order, order), 0)
    col = lax.broadcasted_iota(jnp.int32, (order, order), 1)
    on_diag = row == col
    pivots = jnp.where(on_diag, matrix, 0.0)
    recip_col = 1.0 / jnp.sum(pivots, axis=1, keepdims=True)
    recip_row = 1.0 / jnp.sum(pivots, axis=0, keepdims=True)
    power = -(recip_col * jnp.where(col > row, matrix, 0.0))
    identity = jnp.where(on_diag, 1.0, 0.0)
    product = identity + power
    steps = max((order - 1).bit_length(), 1)
    for level in range(steps - 1):
        power = dot(power, power)
        product = dot(product, identity + power)
    return product * recip_row


def split(value):
    high = value.astype(jnp.bfloat16)
    low = (value - high.astype(jnp.float32)).astype(jnp.bfloat16)
    return high, low


def kernel(n_mc, n_mr, chunks, tile,
           column_ref, diag_ref, row_ref, trailing_ref,
           solved_ref, inverse_ref, scaled_ref, updated_ref,
           panel, columns, diags, matrix, flipped, left_high, left_low,
           load_sem, trail_sem, send_sem, recv_sem,
           diag_send, diag_recv, block_send, block_recv, col_send, col_recv):
    mc = lax.axis_index("mc")
    mr = lax.axis_index("mr")
    levels = n_mc // 2
    z = mc // 2
    x = lax.rem(mc, 2)
    rows = row_ref.shape[0]
    half = rows // 2
    cols = row_ref.shape[1]
    width = cols // chunks
    block_cols = diag_ref.shape[1]
    height = column_ref.shape[1]

    def at(mc_index, mr_index):
        return {"mc": mc_index, "mr": mr_index}

    own_row = pltpu.make_async_copy(
        row_ref, panel.at[pl.ds(pl.multiple_of(mc * rows, rows), rows)], load_sem.at[0])
    own_diag = pltpu.make_async_copy(
        diag_ref, diags.at[mr, pl.ds(pl.multiple_of(mc * rows, rows), rows)], load_sem.at[1])
    own_part = lambda k: pl.ds(pl.multiple_of(k * block_cols, block_cols), block_cols)
    own_column = pltpu.make_async_copy(column_ref, columns.at[own_part(mr)], load_sem.at[2])
    own_row.start()
    own_diag.start()
    own_column.start()

    barrier = pltpu.get_barrier_semaphore()
    for step in range(1, n_mc):
        pl.semaphore_signal(barrier, inc=1, device_id=at(lax.rem(mc + step, n_mc), mr),
                            device_id_type=pl.DeviceIdType.MESH)
    for step in range(1, n_mr):
        pl.semaphore_signal(barrier, inc=1, device_id=at(mc, lax.rem(mr + step, n_mr)),
                            device_id_type=pl.DeviceIdType.MESH)
    pl.semaphore_wait(barrier, n_mc + n_mr - 2)

    def piece(shard, c, low=None):
        first = pl.multiple_of(shard * rows, rows)
        count = rows
        if low is not None:
            first = pl.multiple_of(shard * rows + low * half, half)
            count = half
        return panel.at[pl.ds(first, count), pl.ds(pl.multiple_of(c * width, width), width)]

    def copy(shard, c, way, slot, target, low=None):
        ref = piece(shard, c, low)
        return pltpu.make_async_remote_copy(
            src_ref=ref, dst_ref=ref,
            send_sem=send_sem.at[way, slot, c],
            recv_sem=recv_sem.at[2 * shard + (1 if low == 1 else 0), c],
            device_id=at(target, mr), device_id_type=pl.DeviceIdType.MESH)

    down = jnp.maximum(mc - 2, 0)
    up = jnp.minimum(mc + 2, n_mc - 1)
    across = z * 2 + 1 - x

    def diag_copy(step, source, target):
        ref = diags.at[mr, pl.ds(pl.multiple_of(source * rows, rows), rows)]
        return pltpu.make_async_remote_copy(
            src_ref=ref, dst_ref=ref, send_sem=diag_send.at[step], recv_sem=diag_recv.at[step],
            device_id=at(target, mr), device_id_type=pl.DeviceIdType.MESH)

    def block_copy(step, source, target):
        ref = diags.at[source]
        return pltpu.make_async_remote_copy(
            src_ref=ref, dst_ref=ref, send_sem=block_send.at[step], recv_sem=block_recv.at[step],
            device_id=at(mc, target), device_id_type=pl.DeviceIdType.MESH)

    def column_copy(step, source, target):
        ref = columns.at[own_part(source)]
        return pltpu.make_async_remote_copy(
            src_ref=ref, dst_ref=ref, send_sem=col_send.at[step], recv_sem=col_recv.at[step],
            device_id=at(mc, target), device_id_type=pl.DeviceIdType.MESH)

    own_diag.wait()
    for step in range(1, n_mc):
        diag_copy(step, mc, lax.rem(mc + step, n_mc)).start()
    own_row.wait()

    @pl.loop(0, chunks)
    def _(c):
        @pl.when(z > 0)
        def _():
            copy(mc, c, 0, z, down).start()

        @pl.when(z < levels - 1)
        def _():
            copy(mc, c, 1, z, up).start()

        copy(mc, c, 2, z, across).start()

    own_column.wait()
    for step in range(1, n_mr):
        column_copy(step, mr, lax.rem(mr + step, n_mr)).start()

    def trail_copy(c):
        part = pl.ds(pl.multiple_of(c * width, width), width)
        return pltpu.make_async_copy(trailing_ref.at[:, part], updated_ref.at[:, part], trail_sem.at[c])

    @pl.loop(0, chunks)
    def _(c):
        trail_copy(c).start()

    for step in range(1, n_mc):
        diag_copy(step, lax.rem(mc + n_mc - step, n_mc), lax.rem(mc + step, n_mc)).wait_recv()
    for step in range(1, n_mr):
        block_copy(step, mr, lax.rem(mr + step, n_mr)).start()
    for step in range(1, n_mr):
        block_copy(step, lax.rem(mr + n_mr - step, n_mr), lax.rem(mr + step, n_mr)).wait_recv()
    for k in range(n_mr):
        matrix[:, k * block_cols:(k + 1) * block_cols] = diags[k]
    matrix[...] = upper_inverse(matrix[...])
    own_inverse = matrix[pl.ds(pl.multiple_of(mc * rows, rows), rows), :]
    for step in range(1, n_mr):
        column_copy(step, lax.rem(mr + n_mr - step, n_mr), lax.rem(mr + step, n_mr)).wait_recv()
    flipped[...] = -lax.dot_general(
        matrix[...], columns[...], (((0,), (0,)), ((), ())),
        precision=HIGHEST, preferred_element_type=jnp.float32)
    solved_ref[...] = flipped[own_part(mr), :]
    left_high[0:height, :], left_low[0:height, :] = split(flipped[...].T)
    left_high[height:height + rows, :], left_low[height:height + rows, :] = split(own_inverse)
    for k in range(n_mr):
        @pl.when(mr == k)
        def _():
            inverse_ref[...] = own_inverse[:, k * block_cols:(k + 1) * block_cols]

    first_half_only = lambda q: jnp.logical_or(
        jnp.logical_and(q == levels - 1, z != levels - 1), jnp.logical_and(q == 0, z != 0))

    def each_across(q, c, act):
        @pl.when(first_half_only(q))
        def _():
            act(copy(2 * q + x, c, 2, q, across, 0))

        @pl.when(jnp.logical_not(first_half_only(q)))
        def _():
            act(copy(2 * q + x, c, 2, q, across))

    start = lambda d: d.start()
    other = 1 - x
    top = 2 * (levels - 1) + other
    bottom = other

    for phase in range(levels - 1):
        above = z + 1 + phase
        below = z - 1 - phase

        @pl.loop(0, chunks)
        def _(c):
            @pl.when(above < levels)
            def _():
                copy(2 * above + x, c, 0, above, down).wait_recv()

                @pl.when(z > 0)
                def _():
                    copy(2 * above + x, c, 0, above, down).start()

                each_across(above, c, start)

            @pl.when(below >= 0)
            def _():
                copy(2 * below + x, c, 1, below, up).wait_recv()

                @pl.when(z < levels - 1)
                def _():
                    copy(2 * below + x, c, 1, below, up).start()

                each_across(below, c, start)

            if phase == 0:
                copy(2 * z + other, c, 2, z, across).wait_recv()

                @pl.when(z == levels - 1)
                def _():
                    copy(top, c, 0, levels, down, 1).start()

                @pl.when(z == 0)
                def _():
                    copy(bottom, c, 1, levels, up, 1).start()

            @pl.when(above == levels)
            def _():
                @pl.when(z < levels - 1)
                def _():
                    copy(top, c, 0, levels, down, 1).wait_recv()

                    @pl.when(z > 0)
                    def _():
                        copy(top, c, 0, levels, down, 1).start()

            @pl.when(below == -1)
            def _():
                @pl.when(z > 0)
                def _():
                    copy(bottom, c, 1, levels, up, 1).wait_recv()

                    @pl.when(z < levels - 1)
                    def _():
                        copy(bottom, c, 1, levels, up, 1).start()

    @pl.loop(0, chunks)
    def _(c):
        trail_copy(c).wait()

        @pl.when(z == 0)
        def _():
            copy(top, c, 0, levels, down, 1).wait_recv()

        @pl.when(z == levels - 1)
        def _():
            copy(bottom, c, 1, levels, up, 1).wait_recv()

        for q in range(levels):
            def receive(low):
                copy(2 * q + other, c, 2, q, across, low).wait_recv()

            @pl.when(jnp.logical_and(z != q, first_half_only(q)))
            def _():
                receive(0)

            @pl.when(jnp.logical_and(z != q, jnp.logical_not(first_half_only(q))))
            def _():
                receive(None)

        for t in range(width // tile):
            part = pl.ds(pl.multiple_of(c * width + t * tile, tile), tile)
            right_high, right_low = split(panel[:, part])
            product = jnp.dot(left_high[...], right_low, preferred_element_type=jnp.float32)
            product += jnp.dot(left_low[...], right_high, preferred_element_type=jnp.float32)
            product += jnp.dot(left_high[...], right_high, preferred_element_type=jnp.float32)
            updated_ref[:, part] = updated_ref[:, part] + product[0:height]
            scaled_ref[:, part] = product[height:height + rows]

    for step in range(1, n_mc):
        diag_copy(step, mc, lax.rem(mc + step, n_mc)).wait_send()
    for step in range(1, n_mr):
        block_copy(step, mr, lax.rem(mr + step, n_mr)).wait_send()
        column_copy(step, mr, lax.rem(mr + step, n_mr)).wait_send()

    @pl.loop(0, chunks)
    def _(c):
        for q in range(levels):
            @pl.when(jnp.logical_and(z > 0, z <= q))
            def _():
                copy(2 * q + x, c, 0, q, down).wait_send()

            @pl.when(jnp.logical_and(z < levels - 1, z >= q))
            def _():
                copy(2 * q + x, c, 1, q, up).wait_send()

            each_across(q, c, lambda d: d.wait_send())

        @pl.when(z > 0)
        def _():
            copy(top, c, 0, levels, down, 1).wait_send()

        @pl.when(z < levels - 1)
        def _():
            copy(bottom, c, 1, levels, up, 1).wait_send()


def store(*refs):
    n = len(refs) // 2
    copies = [pltpu.make_async_copy(refs[i], refs[n + i], refs[-1].at[i]) for i in range(n)]
    for c in copies:
        c.start()
    for c in copies:
        c.wait()


def shards(n_mc, n_mr, column_panel, diag_block, row_panel, trailing):
    rows, block_cols = diag_block.shape
    height, cols = trailing.shape
    order = rows * n_mc
    levels = n_mc // 2
    chunks = max(1, 32 // levels)
    while cols % (chunks * 128):
        chunks //= 2
    width = cols // chunks
    tile = 512 if width % 512 == 0 else 128
    dma = pltpu.SemaphoreType.DMA
    f32 = jnp.float32
    anywhere = pl.BlockSpec(memory_space=pl.ANY)
    vmem = pl.BlockSpec(memory_space=pltpu.VMEM)
    parts = pl.pallas_call(
        functools.partial(kernel, n_mc, n_mr, chunks, tile),
        out_shape=(
            pltpu.VMEM((block_cols, height), f32),
            pltpu.VMEM(diag_block.shape, f32),
            pltpu.VMEM(row_panel.shape, f32),
            pltpu.VMEM(trailing.shape, f32),
        ),
        in_specs=[pl.BlockSpec(memory_space=pltpu.HBM)] * 4,
        out_specs=(vmem,) * 4,
        scratch_shapes=[
            pltpu.VMEM((order, cols), f32),
            pltpu.VMEM((order, height), f32),
            pltpu.VMEM((n_mr, order, block_cols), f32),
            pltpu.VMEM((order, order), f32),
            pltpu.VMEM((order, height), f32),
            pltpu.VMEM((height + rows, order), jnp.bfloat16),
            pltpu.VMEM((height + rows, order), jnp.bfloat16),
            dma((3,)), dma((chunks,)),
            dma((3, levels + 1, chunks)), dma((2 * n_mc, chunks)),
            dma((n_mc,)), dma((n_mc,)), dma((n_mr,)), dma((n_mr,)), dma((n_mr,)), dma((n_mr,)),
        ],
        compiler_params=pltpu.CompilerParams(
            collective_id=0, has_side_effects=True, vmem_limit_bytes=26 * 1024 * 1024),
    )(column_panel.T, diag_block, row_panel, trailing)
    solved, inverse, scaled, updated = pl.pallas_call(
        store,
        out_shape=tuple(jax.ShapeDtypeStruct(part.shape, f32) for part in parts),
        in_specs=[vmem] * 4,
        out_specs=(anywhere,) * 4,
        scratch_shapes=[dma((4,))],
        compiler_params=pltpu.CompilerParams(vmem_limit_bytes=1024 * 1024),
    )(*parts)
    return solved.T, inverse, scaled, updated


def solution(mesh):
    placed = (P("mc", "mr"),) * 4
    return jax.shard_map(
        functools.partial(shards, mesh.shape["mc"], mesh.shape["mr"]),
        mesh=mesh, in_specs=placed, out_specs=placed, check_vma=False)
```

```python
import functools

import jax
import jax.numpy as jnp
from jax import lax
from jax.experimental import pallas as pl
from jax.experimental.pallas import tpu as pltpu
from jax.sharding import PartitionSpec as P

VMEM_BYTES = 67043328
HIGHEST = lax.Precision.HIGHEST


def dot(a, b):
    return jnp.dot(a, b, precision=HIGHEST, preferred_element_type=jnp.float32)


def upper_inverse(matrix):
    order = matrix.shape[0]
    row = lax.broadcasted_iota(jnp.int32, (order, order), 0)
    col = lax.broadcasted_iota(jnp.int32, (order, order), 1)
    on_diag = row == col
    pivots = jnp.where(on_diag, matrix, 0.0)
    recip_col = 1.0 / jnp.sum(pivots, axis=1, keepdims=True)
    recip_row = 1.0 / jnp.sum(pivots, axis=0, keepdims=True)
    power = -(recip_col * jnp.where(col > row, matrix, 0.0))
    identity = jnp.where(on_diag, 1.0, 0.0)
    product = identity + power
    steps = max((order - 1).bit_length(), 1)
    for level in range(steps - 1):
        power = dot(power, power)
        product = dot(product, identity + power)
    return product * recip_row


def split(value):
    high = value.astype(jnp.bfloat16)
    low = (value - high.astype(jnp.float32)).astype(jnp.bfloat16)
    return high, low


def kernel(n_mc, n_mr, chunks, tile,
           column_ref, diag_ref, row_ref, trailing_ref,
           solved_ref, inverse_ref, scaled_ref, updated_ref,
           panel, columns, diags, matrix, flipped, left_high, left_low,
           load_sem, trail_sem, send_sem, recv_sem,
           diag_send, diag_recv, block_send, block_recv, col_send, col_recv):
    mc = lax.axis_index("mc")
    mr = lax.axis_index("mr")
    levels = n_mc // 2
    z = mc // 2
    x = lax.rem(mc, 2)
    rows = row_ref.shape[0]
    half = rows // 2
    cols = row_ref.shape[1]
    width = cols // chunks
    block_cols = diag_ref.shape[1]
    height = column_ref.shape[1]

    def at(mc_index, mr_index):
        return {"mc": mc_index, "mr": mr_index}

    own_row = pltpu.make_async_copy(
        row_ref, panel.at[pl.ds(pl.multiple_of(mc * rows, rows), rows)], load_sem.at[0])
    own_diag = pltpu.make_async_copy(
        diag_ref, diags.at[mr, pl.ds(pl.multiple_of(mc * rows, rows), rows)], load_sem.at[1])
    own_part = lambda k: pl.ds(pl.multiple_of(k * block_cols, block_cols), block_cols)
    own_column = pltpu.make_async_copy(column_ref, columns.at[own_part(mr)], load_sem.at[2])
    own_row.start()
    own_diag.start()
    own_column.start()

    barrier = pltpu.get_barrier_semaphore()
    for step in range(1, n_mc):
        pl.semaphore_signal(barrier, inc=1, device_id=at(lax.rem(mc + step, n_mc), mr),
                            device_id_type=pl.DeviceIdType.MESH)
    for step in range(1, n_mr):
        pl.semaphore_signal(barrier, inc=1, device_id=at(mc, lax.rem(mr + step, n_mr)),
                            device_id_type=pl.DeviceIdType.MESH)
    pl.semaphore_wait(barrier, n_mc + n_mr - 2)

    def piece(shard, c, low=None):
        first = pl.multiple_of(shard * rows, rows)
        count = rows
        if low is not None:
            first = pl.multiple_of(shard * rows + low * half, half)
            count = half
        return panel.at[pl.ds(first, count), pl.ds(pl.multiple_of(c * width, width), width)]

    def copy(shard, c, way, slot, target, low=None):
        ref = piece(shard, c, low)
        return pltpu.make_async_remote_copy(
            src_ref=ref, dst_ref=ref,
            send_sem=send_sem.at[way, slot, c],
            recv_sem=recv_sem.at[2 * shard + (1 if low == 1 else 0), c],
            device_id=at(target, mr), device_id_type=pl.DeviceIdType.MESH)

    down = jnp.maximum(mc - 2, 0)
    up = jnp.minimum(mc + 2, n_mc - 1)
    across = z * 2 + 1 - x

    def diag_copy(step, source, target):
        ref = diags.at[mr, pl.ds(pl.multiple_of(source * rows, rows), rows)]
        return pltpu.make_async_remote_copy(
            src_ref=ref, dst_ref=ref, send_sem=diag_send.at[step], recv_sem=diag_recv.at[step],
            device_id=at(target, mr), device_id_type=pl.DeviceIdType.MESH)

    def block_copy(step, source, target):
        ref = diags.at[source]
        return pltpu.make_async_remote_copy(
            src_ref=ref, dst_ref=ref, send_sem=block_send.at[step], recv_sem=block_recv.at[step],
            device_id=at(mc, target), device_id_type=pl.DeviceIdType.MESH)

    def column_copy(step, source, target):
        ref = columns.at[own_part(source)]
        return pltpu.make_async_remote_copy(
            src_ref=ref, dst_ref=ref, send_sem=col_send.at[step], recv_sem=col_recv.at[step],
            device_id=at(mc, target), device_id_type=pl.DeviceIdType.MESH)

    own_row.wait()

    @pl.loop(0, chunks)
    def _(c):
        @pl.when(z > 0)
        def _():
            copy(mc, c, 0, z, down).start()

        @pl.when(z < levels - 1)
        def _():
            copy(mc, c, 1, z, up).start()

        copy(mc, c, 2, z, across).start()

    own_diag.wait()
    for step in range(1, n_mc):
        diag_copy(step, mc, lax.rem(mc + step, n_mc)).start()

    own_column.wait()
    for step in range(1, n_mr):
        column_copy(step, mr, lax.rem(mr + step, n_mr)).start()

    def trail_copy(c):
        part = pl.ds(pl.multiple_of(c * width, width), width)
        return pltpu.make_async_copy(trailing_ref.at[:, part], updated_ref.at[:, part], trail_sem.at[c])

    @pl.loop(0, chunks)
    def _(c):
        trail_copy(c).start()

    first_half_only = lambda q: jnp.logical_or(
        jnp.logical_and(q == levels - 1, z != levels - 1), jnp.logical_and(q == 0, z != 0))

    def each_across(q, c, act):
        @pl.when(first_half_only(q))
        def _():
            act(copy(2 * q + x, c, 2, q, across, 0))

        @pl.when(jnp.logical_not(first_half_only(q)))
        def _():
            act(copy(2 * q + x, c, 2, q, across))

    start = lambda d: d.start()
    other = 1 - x
    top = 2 * (levels - 1) + other
    bottom = other

    def invert():
        for step in range(1, n_mc):
            diag_copy(step, lax.rem(mc + n_mc - step, n_mc), lax.rem(mc + step, n_mc)).wait_recv()
        for step in range(1, n_mr):
            block_copy(step, mr, lax.rem(mr + step, n_mr)).start()
        for step in range(1, n_mr):
            block_copy(step, lax.rem(mr + n_mr - step, n_mr), lax.rem(mr + step, n_mr)).wait_recv()
        for k in range(n_mr):
            matrix[:, k * block_cols:(k + 1) * block_cols] = diags[k]
        matrix[...] = upper_inverse(matrix[...])
        own_inverse = matrix[pl.ds(pl.multiple_of(mc * rows, rows), rows), :]
        for step in range(1, n_mr):
            column_copy(step, lax.rem(mr + n_mr - step, n_mr), lax.rem(mr + step, n_mr)).wait_recv()
        flipped[...] = -lax.dot_general(
            matrix[...], columns[...], (((0,), (0,)), ((), ())),
            precision=HIGHEST, preferred_element_type=jnp.float32)
        solved_ref[...] = flipped[own_part(mr), :]
        left_high[0:height, :], left_low[0:height, :] = split(flipped[...].T)
        left_high[height:height + rows, :], left_low[height:height + rows, :] = split(own_inverse)
        for k in range(n_mr):
            @pl.when(mr == k)
            def _():
                inverse_ref[...] = own_inverse[:, k * block_cols:(k + 1) * block_cols]

    for phase in range(levels - 1):
        if phase == min(1, levels - 2):
            invert()

        above = z + 1 + phase
        below = z - 1 - phase

        @pl.loop(0, chunks)
        def _(c):
            @pl.when(above < levels)
            def _():
                copy(2 * above + x, c, 0, above, down).wait_recv()

                @pl.when(z > 0)
                def _():
                    copy(2 * above + x, c, 0, above, down).start()

                each_across(above, c, start)

            @pl.when(below >= 0)
            def _():
                copy(2 * below + x, c, 1, below, up).wait_recv()

                @pl.when(z < levels - 1)
                def _():
                    copy(2 * below + x, c, 1, below, up).start()

                each_across(below, c, start)

            if phase == 0:
                copy(2 * z + other, c, 2, z, across).wait_recv()

                @pl.when(z == levels - 1)
                def _():
                    copy(top, c, 0, levels, down, 1).start()

                @pl.when(z == 0)
                def _():
                    copy(bottom, c, 1, levels, up, 1).start()

            @pl.when(above == levels)
            def _():
                @pl.when(z < levels - 1)
                def _():
                    copy(top, c, 0, levels, down, 1).wait_recv()

                    @pl.when(z > 0)
                    def _():
                        copy(top, c, 0, levels, down, 1).start()

            @pl.when(below == -1)
            def _():
                @pl.when(z > 0)
                def _():
                    copy(bottom, c, 1, levels, up, 1).wait_recv()

                    @pl.when(z < levels - 1)
                    def _():
                        copy(bottom, c, 1, levels, up, 1).start()

    @pl.loop(0, chunks)
    def _(c):
        trail_copy(c).wait()

        @pl.when(z == 0)
        def _():
            copy(top, c, 0, levels, down, 1).wait_recv()

        @pl.when(z == levels - 1)
        def _():
            copy(bottom, c, 1, levels, up, 1).wait_recv()

        for q in range(levels):
            def receive(low):
                copy(2 * q + other, c, 2, q, across, low).wait_recv()

            @pl.when(jnp.logical_and(z != q, first_half_only(q)))
            def _():
                receive(0)

            @pl.when(jnp.logical_and(z != q, jnp.logical_not(first_half_only(q))))
            def _():
                receive(None)

        for t in range(width // tile):
            part = pl.ds(pl.multiple_of(c * width + t * tile, tile), tile)
            right_high, right_low = split(panel[:, part])
            product = jnp.dot(left_high[...], right_low, preferred_element_type=jnp.float32)
            product += jnp.dot(left_low[...], right_high, preferred_element_type=jnp.float32)
            product += jnp.dot(left_high[...], right_high, preferred_element_type=jnp.float32)
            updated_ref[:, part] = updated_ref[:, part] + product[0:height]
            scaled_ref[:, part] = product[height:height + rows]

    for step in range(1, n_mc):
        diag_copy(step, mc, lax.rem(mc + step, n_mc)).wait_send()
    for step in range(1, n_mr):
        block_copy(step, mr, lax.rem(mr + step, n_mr)).wait_send()
        column_copy(step, mr, lax.rem(mr + step, n_mr)).wait_send()

    @pl.loop(0, chunks)
    def _(c):
        for q in range(levels):
            @pl.when(jnp.logical_and(z > 0, z <= q))
            def _():
                copy(2 * q + x, c, 0, q, down).wait_send()

            @pl.when(jnp.logical_and(z < levels - 1, z >= q))
            def _():
                copy(2 * q + x, c, 1, q, up).wait_send()

            each_across(q, c, lambda d: d.wait_send())

        @pl.when(z > 0)
        def _():
            copy(top, c, 0, levels, down, 1).wait_send()

        @pl.when(z < levels - 1)
        def _():
            copy(bottom, c, 1, levels, up, 1).wait_send()


def store(*refs):
    sources, targets, sem = refs[:4], refs[4:8], refs[8]
    strips = sem.shape[0] - 3
    deep = sources[3].shape[0] // strips
    copies = []
    for i in range(strips):
        part = pl.ds(i * deep, deep)
        copies.append(pltpu.make_async_copy(sources[3].at[part], targets[3].at[part], sem.at[3 + i]))
    for i in range(3):
        copies.append(pltpu.make_async_copy(sources[i], targets[i], sem.at[i]))
    for c in copies:
        c.start()
    for c in copies:
        c.wait()


def shards(n_mc, n_mr, column_panel, diag_block, row_panel, trailing):
    rows, block_cols = diag_block.shape
    height, cols = trailing.shape
    order = rows * n_mc
    levels = n_mc // 2
    chunks = max(1, 16 // levels)
    while cols % (chunks * 128):
        chunks //= 2
    width = cols // chunks
    tile = 512 if width % 512 == 0 else 128
    held = 4 * (height * cols + rows * cols + block_cols * height + rows * 128) + 64 * 1024
    dma = pltpu.SemaphoreType.DMA
    f32 = jnp.float32
    anywhere = pl.BlockSpec(memory_space=pl.ANY)
    vmem = pl.BlockSpec(memory_space=pltpu.VMEM)
    parts = pl.pallas_call(
        functools.partial(kernel, n_mc, n_mr, chunks, tile),
        out_shape=(
            pltpu.VMEM((block_cols, height), f32),
            pltpu.VMEM(diag_block.shape, f32),
            pltpu.VMEM(row_panel.shape, f32),
            pltpu.VMEM(trailing.shape, f32),
        ),
        in_specs=[pl.BlockSpec(memory_space=pltpu.HBM)] * 4,
        out_specs=(vmem,) * 4,
        scratch_shapes=[
            pltpu.VMEM((order, cols), f32),
            pltpu.VMEM((order, height), f32),
            pltpu.VMEM((n_mr, order, block_cols), f32),
            pltpu.VMEM((order, order), f32),
            pltpu.VMEM((order, height), f32),
            pltpu.VMEM((height + rows, order), jnp.bfloat16),
            pltpu.VMEM((height + rows, order), jnp.bfloat16),
            dma((3,)), dma((chunks,)),
            dma((3, levels + 1, chunks)), dma((2 * n_mc, chunks)),
            dma((n_mc,)), dma((n_mc,)), dma((n_mr,)), dma((n_mr,)), dma((n_mr,)), dma((n_mr,)),
        ],
        compiler_params=pltpu.CompilerParams(
            collective_id=0, has_side_effects=True, vmem_limit_bytes=VMEM_BYTES - held),
    )(column_panel.T, diag_block, row_panel, trailing)
    solved, inverse, scaled, updated = pl.pallas_call(
        store,
        out_shape=tuple(jax.ShapeDtypeStruct(part.shape, f32) for part in parts),
        in_specs=[vmem] * 4,
        out_specs=(anywhere,) * 4,
        scratch_shapes=[dma((3 + 8,))],
        compiler_params=pltpu.CompilerParams(vmem_limit_bytes=1024 * 1024),
    )(*parts)
    return solved.T, inverse, scaled, updated


def solution(mesh):
    placed = (P("mc", "mr"),) * 4
    return jax.shard_map(
        functools.partial(shards, mesh.shape["mc"], mesh.shape["mr"]),
        mesh=mesh, in_specs=placed, out_specs=placed, check_vma=False)
```
